512 devices in a mesh: seq: 64 (over z, y), head: 8 (over x, core).
Axes of the slice: x: 4, y: 4, z: 16, core: 2. Of those that a mesh axis runs over, the one named last changes fastest.
Arguments:
- queries: bfloat16 [8192, 16, 128], P('seq', 'head'), may hold values from -6 to 6
- key_vectors: bfloat16 [8192, 16, 128], P('seq', 'head'), may hold values from -16 to 16
- values: bfloat16 [8192, 16, 128], P('seq', 'head'), may hold values from -6 to 6
- out_gate: bfloat16 [8192, 16, 128], P('seq', 'head'), may hold values from -6 to 6
- inputs: bfloat16 [8192, 2048], P('seq', 'head'), may hold values from -6 to 6
- beta_weight: bfloat16 [16, 2048], P(None, 'head'), may hold values from -0.1875 to 0.1875
- log_decay: float32 [16, 8192], P('head', 'seq'), may hold values from -1 to 0
- initial_state: float32 [16, 128, 128], P('head'), may hold values from -6 to 6
Outputs:
- gated_out: bfloat16 [8192, 16, 128], P('seq', 'head')
- block_states: float32 [128, 16, 128, 128], P('seq', 'head')
The draws below stay inside these ranges and needn't reach their ends.
All inputs are finite; a program needn't handle non-finite values.
Results may differ from the reference program's by a relative error of at most 0.0012.
Values sent between devices are 32-bit elements; how exact they have to be, the bound alone decides.
A program may use at most 64 MiB of HBM per device.

```python
import math
import jax
import jax.numpy as jnp
from jax import lax

D = 2048
HEADS = 16
HEAD_DIM = 128
BLOCK = 64
TOK_DEV = 128
SEQUENCE_TOKENS = 8192


def gradual_heads(key, slow_count):
    ranking = jax.random.permutation(jax.random.fold_in(key, 41), HEADS)
    return ranking < slow_count


def draw_key_vectors(key, part):
    rough_key = jax.random.fold_in(jax.random.fold_in(key, 17), 0)
    entry_key = jax.random.fold_in(jax.random.fold_in(key, 17), 1)
    basis_key = jax.random.fold_in(jax.random.fold_in(key, 17), 3)
    position = jnp.arange(SEQUENCE_TOKENS, dtype=jnp.float32)
    rising = jnp.sqrt(1.0 + 2.0 * position / SEQUENCE_TOKENS)[:, None, None]
    roughness = jnp.exp(jax.random.uniform(rough_key, (SEQUENCE_TOKENS, HEADS, 1), minval=-1.2, maxval=1.2))
    slow_count = HEADS // 2
    entries = jax.random.normal(entry_key, (SEQUENCE_TOKENS, HEADS, HEAD_DIM), dtype=jnp.float32)
    gradual = gradual_heads(key, slow_count)
    orders = jax.vmap(lambda head_key: jax.random.permutation(head_key, HEAD_DIM))(jax.random.split(basis_key, HEADS))
    inside = orders < HEAD_DIM // 4
    leakage = math.sqrt(HEAD_DIM / (4.0 * SEQUENCE_TOKENS))
    column_scale = jnp.where(jnp.logical_or(inside, jnp.logical_not(gradual[:, None])), 1.0, leakage)
    return jnp.clip(entries * column_scale[None] * roughness * rising, -16.0, 16.0).astype(jnp.bfloat16)


def draw_log_decay(key, part):
    slow_key = jax.random.fold_in(jax.random.fold_in(key, 29), 1)
    fast_key = jax.random.fold_in(jax.random.fold_in(key, 29), 2)
    token_key = jax.random.fold_in(jax.random.fold_in(key, 29), 3)
    block_key = jax.random.fold_in(jax.random.fold_in(key, 29), 4)
    place_key = jax.random.fold_in(jax.random.fold_in(key, 29), 5)
    depth_key = jax.random.fold_in(jax.random.fold_in(key, 29), 6)
    slow_count = HEADS // 2
    gradual = gradual_heads(key, slow_count)[:, None]
    slow_rate = jnp.exp(jax.random.uniform(slow_key, (HEADS, 1), minval=math.log(0.05 / SEQUENCE_TOKENS), maxval=math.log(0.5 / SEQUENCE_TOKENS)))
    fast_rate = jnp.exp(jax.random.uniform(fast_key, (HEADS, 1), minval=math.log(1.0 / 50.0), maxval=math.log(1.0 / 30.0)))
    baseline_decay_rate = jnp.where(gradual, slow_rate, fast_rate)
    token_scale_factor = jnp.exp(jax.random.uniform(token_key, (HEADS, SEQUENCE_TOKENS), minval=-0.7, maxval=0.7))
    block_scale_factor = jnp.repeat(jnp.exp(jax.random.uniform(block_key, (HEADS, SEQUENCE_TOKENS // TOK_DEV), minval=-0.7, maxval=0.7)), TOK_DEV, axis=1)
    spike_positions = jax.random.randint(place_key, (3,), 0, SEQUENCE_TOKENS)
    decay_depths = jax.random.uniform(depth_key, (3, HEADS), minval=0.2, maxval=0.5)
    spike_region_mask = (jnp.arange(SEQUENCE_TOKENS)[None, :] == spike_positions[:, None]).astype(jnp.float32)
    spike_regions = jnp.einsum('gn,gs->ns', jnp.log(1.0 - decay_depths), spike_region_mask)
    return -baseline_decay_rate * token_scale_factor * block_scale_factor + jnp.where(gradual, spike_regions, 0.0)


def spiked(values, own_key, source, target, blocks, factor):
    def block_of(axis_at):
        return (jnp.arange(values.shape[axis_at]) // (values.shape[axis_at] // blocks)).reshape((-1,) + (1,) * (values.ndim - 1 - axis_at))

    one_side = jax.random.permutation(own_key, blocks)[block_of(target)]
    second = (block_of(target) + blocks // 2) % blocks
    return jnp.where((block_of(source) == one_side) | (block_of(source) == second), factor * values, values)


def steps_of(own_key, extent, cuts, low, largest):
    level = 1.0
    for axis_at, blocks in cuts:
        heights = jax.random.uniform(jax.random.fold_in(jax.random.fold_in(own_key, 6), axis_at), (blocks,), jnp.float32, low / len(cuts), largest / len(cuts))
        level = level * jnp.repeat(jnp.exp(heights), extent[axis_at] // blocks).reshape((-1,) + (1,) * (len(extent) - 1 - axis_at))
    return level


def bell_draw(key, dims, width, most, pieces=(), kind=jnp.bfloat16):
    drawn = width * jax.random.normal(key, dims, jnp.float32)
    if pieces:
        drawn = drawn * steps_of(key, dims, pieces, -0.22, 0.18)
    return jnp.clip(drawn, -most, most).astype(kind)


def gaussian_with(key, dims, scale, limit, cuts, heavy, held_as=jnp.bfloat16):
    array = scale * jax.random.normal(key, dims, jnp.float32)
    if cuts:
        array = array * steps_of(key, dims, cuts, -0.22, 0.18)
    return jnp.clip(spiked(array, jax.random.fold_in(key, 3), *heavy), -limit, limit).astype(held_as)


def setup_inputs(seed: int = 0) -> dict:
    key_list = jax.random.split(jax.random.key(seed), 9)
    return {
        "queries": bell_draw(key_list[0], (SEQUENCE_TOKENS, HEADS, HEAD_DIM), 1.0, 6.0, ((0, 64), (1, 8))),
        "key_vectors": draw_key_vectors(jax.random.fold_in(key_list[8], 71), 0),
        "values": bell_draw(key_list[2], (SEQUENCE_TOKENS, HEADS, HEAD_DIM), 1.0, 6.0, ((0, 64), (1, 8))),
        "out_gate": bell_draw(key_list[3], (SEQUENCE_TOKENS, HEADS, HEAD_DIM), 1.0, 6.0, ((0, 64), (1, 8))),
        "inputs": bell_draw(key_list[4], (SEQUENCE_TOKENS, D), 1.0, 6.0, ((0, 64), (1, 8))),
        "beta_weight": gaussian_with(key_list[5], (HEADS, D), D ** -0.5, 0.1875, ((1, 8),), (1, 0, 8, 2.0)),
        "log_decay": draw_log_decay(jax.random.fold_in(key_list[8], 71), 0),
        "initial_state": bell_draw(key_list[7], (HEADS, HEAD_DIM, HEAD_DIM), 1.0, 6.0, ((0, 8),), jnp.float32),
    }


EPSILON = 1e-06

def matmul(matrix, operand):
    return jnp.einsum('...ij,...jk->...ik', matrix, operand, precision=lax.Precision.HIGHEST)

def normalize(query_block, key_block, key_limit):
    query_float = query_block.astype(jnp.float32)
    key_float = key_block.astype(jnp.float32)
    queries_unit = query_float / jnp.sqrt(lax.optimization_barrier(jnp.sum(query_float * query_float, -1, keepdims=True)) + EPSILON) * query_float.shape[-1] ** (-0.5)
    keys_unit = key_float / jnp.maximum(jnp.sqrt(lax.optimization_barrier(jnp.sum(key_float * key_float, -1, keepdims=True))), key_limit)
    return (queries_unit, keys_unit)

def block_parts(queries_unit, keys_unit, value_rows, beta_gate, decay_rows):
    length = decay_rows.shape[-1]
    feature = keys_unit.shape[-1]
    cumulative = jnp.cumsum(decay_rows, axis=-1)
    inside = jnp.tril(jnp.ones((length, length), jnp.float32))
    strict = jnp.tril(jnp.ones((length, length), jnp.float32), -1)
    spread = jnp.where(inside > 0, cumulative[..., :, None] - cumulative[..., None, :], 0.0)
    damping = jnp.exp(spread) * inside
    intersections = jnp.einsum('...id,...jd->...ij', keys_unit, keys_unit, precision=lax.Precision.HIGHEST)
    system = jnp.eye(length, dtype=jnp.float32) + beta_gate[..., :, None] * intersections * damping * strict
    right_side = jnp.concatenate([(beta_gate * jnp.exp(cumulative))[..., None] * keys_unit, beta_gate[..., None] * value_rows], axis=-1)
    solved = lax.linalg.triangular_solve(system, right_side, left_side=True, lower=True, unit_diagonal=True)
    write_keys = solved[..., :feature]
    write_values = solved[..., feature:]
    final_sum = cumulative[..., -1:]
    carried = keys_unit * jnp.exp(final_sum - cumulative)[..., None]
    transition = jnp.exp(final_sum)[..., None] * jnp.eye(feature, dtype=jnp.float32) - jnp.einsum('...ld,...le->...de', carried, write_keys, precision=lax.Precision.HIGHEST)
    offset = jnp.einsum('...ld,...le->...de', carried, write_values, precision=lax.Precision.HIGHEST)
    reached = queries_unit * jnp.exp(cumulative)[..., None]
    scores = jnp.einsum('...id,...jd->...ij', queries_unit, keys_unit, precision=lax.Precision.HIGHEST) * damping
    return (write_keys, write_values, transition, offset, reached, scores)

def block_out(block_info, state_now):
    write_keys, write_values, transition, offset, reached, scores = block_info
    corrected = write_values - matmul(write_keys, state_now)
    return matmul(reached, state_now) + matmul(scores, corrected)

def gate_norm(raw_out, gate_rows):
    inverse_rms = 1.0 / jnp.sqrt(lax.optimization_barrier(jnp.mean(raw_out * raw_out, -1, keepdims=True)) + EPSILON)
    return (raw_out * inverse_rms * jax.nn.silu(gate_rows.astype(jnp.float32))).astype(jnp.bfloat16)

def reference(queries, key_vectors, values, out_gate, inputs, beta_weight, log_decay, initial_state):
    token_count = queries.shape[0]
    head_count = queries.shape[1]
    logits = lax.dot_general(beta_weight.astype(jnp.float32), inputs.astype(jnp.float32), (((1,), (1,)), ((), ())), preferred_element_type=jnp.float32)
    beta_gate = jax.nn.sigmoid(logits)
    key_float = key_vectors.astype(jnp.float32)
    key_total = lax.optimization_barrier(jnp.sum(key_float * key_float, axis=(0, 2)))
    key_limit = jnp.sqrt(key_total / token_count + EPSILON)
    blocks = token_count // BLOCK

    def arrange(tensor):
        return tensor.reshape(blocks, BLOCK, head_count, -1).transpose(0, 2, 1, 3)

    def arrange_rows(tensor):
        return tensor.reshape(head_count, blocks, BLOCK).transpose(1, 0, 2)
    sources = (arrange(queries), arrange(key_vectors), arrange(values), arrange(out_gate), arrange_rows(beta_gate), arrange_rows(log_decay))

    def step(state_now, source):
        query_block, key_block, value_block, gate_block, beta_block, decay_block = source
        queries_unit, keys_unit = normalize(query_block, key_block, key_limit[:, None, None])
        block_info = block_parts(queries_unit, keys_unit, value_block.astype(jnp.float32), beta_block, decay_block)
        raw_out = block_out(block_info, state_now)
        following = matmul(block_info[2], state_now) + block_info[3]
        return (following, (gate_norm(raw_out, gate_block), state_now))
    _, (outputs, states) = lax.scan(step, initial_state.astype(jnp.float32), sources)
    gated_out = outputs.transpose(0, 2, 1, 3).reshape(token_count, head_count, -1)
    return (gated_out, states)
```

```python
import functools

import jax
import jax.numpy as jnp
from jax import lax
from jax.experimental import pallas as pl
from jax.experimental.pallas import tpu as pltpu
from jax.sharding import PartitionSpec as P

MESH = pl.DeviceIdType.MESH
F32 = jnp.float32
BF16 = jnp.bfloat16
EPSILON = 1e-06
Y = 4
Z4 = 4
TOK = 128
HALF = 64
DIM = 128
SL = DIM // Y
NH = 2

NN = (((1,), (0,)), ((), ()))
NT = (((1,), (1,)), ((), ()))


def bdot(a, b, dims):
    return lax.dot_general(a, b, dims, preferred_element_type=F32)


def split(x):
    high = x.astype(BF16)
    return high, (x - high.astype(F32)).astype(BF16)


def mm(a, b, dims=NN):
    ah, al = split(a)
    bh, bl = split(b)
    return bdot(ah, bh, dims) + (bdot(al, bh, dims) + bdot(ah, bl, dims))


def mm_right_exact(a, b, dims=NN):
    ah, al = split(a)
    return bdot(ah, b, dims) + bdot(al, b, dims)


def mm_left_exact(a, b, dims=NN):
    bh, bl = split(b)
    return bdot(a, bh, dims) + bdot(a, bl, dims)


def unit_lower_inverse(strict_part, row, col, eye):
    def same(size):
        return (row // size) == (col // size)

    base = jnp.where(same(8), strict_part, 0.0)
    square = mm(base, base)
    cube = mm(base, square)
    fourth = mm(square, square)
    part = eye - base + square - cube
    inverse = part + mm(part, fourth)
    size = 8
    while size < TOK:
        below = jnp.where(same(2 * size) & jnp.logical_not(same(size)), strict_part, 0.0)
        inverse = inverse - mm(inverse, mm(below, inverse))
        size *= 2
    return inverse


def kernel(
    n_seq,
    n_head,
    q_ref,
    k_ref,
    v_ref,
    gate_ref,
    x_ref,
    w_ref,
    ld_ref,
    s0_ref,
    out_ref,
    st_ref,
    lg,
    lg_in,
    kt,
    kty_in,
    ktz,
    ktz_in,
    ta,
    oa,
    oown,
    et,
    eo,
    b1t,
    b1o,
    b2t,
    b2o,
    pt,
    po,
    p4t,
    p4o,
    ext,
    exo,
    seg_s,
    nxt,
    sd,
    sin,
    s0t,
    r_s,
    c_s,
    t0_s,
    o0_s,
    lg_send,
    lg_recv,
    kty_send,
    kty_recv,
    ktz_send,
    ktz_recv,
    a_send,
    a_recv,
    f_send,
    oa_send,
    oa_recv,
    b_send,
    b_recv,
    seg_send,
    seg_recv,
    sd_send,
    sd_recv,
):
    nz = n_seq // Y
    nseg = nz // Z4
    s = lax.axis_index("seq")
    h = lax.axis_index("head")
    z = s // Y
    y = s % Y
    zl = z % Z4
    seg = z // Z4

    def at_y(d):
        return {"seq": z * Y + (y + d) % Y, "head": h}

    def at_z(d):
        return {"seq": ((z + d) % nz) * Y + y, "head": h}

    def at_head(d):
        return {"seq": s, "head": (h + d) % n_head}

    def rcopy(src, dst, ssem, rsem, dev):
        return pltpu.make_async_remote_copy(
            src_ref=src, dst_ref=dst, send_sem=ssem, recv_sem=rsem, device_id=dev, device_id_type=MESH
        )

    barrier = pltpu.get_barrier_semaphore()
    partners = (
        [at_head(d) for d in range(1, n_head)]
        + [at_y(d) for d in range(1, Y)]
        + [at_z(d) for d in range(1, nz)]
    )
    for dev in partners:
        pl.semaphore_signal(barrier, inc=1, device_id=dev, device_id_type=MESH)

    logits = bdot(w_ref[...], x_ref[...], NT)
    for p in range(n_head):
        lg[p] = logits[NH * p : NH * p + NH]
    ks = [k_ref[:, i, :] for i in range(NH)]
    qs = [q_ref[:, i, :] for i in range(NH)]
    vs = [v_ref[:, i, :] for i in range(NH)]
    ksq = [jnp.sum(jnp.square(k.astype(F32)), axis=1, keepdims=True) for k in ks]
    qsq = [jnp.sum(jnp.square(q.astype(F32)), axis=1, keepdims=True) for q in qs]
    tot = [jnp.sum(a, axis=0, keepdims=True) for a in ksq]
    sub = lax.broadcasted_iota(jnp.int32, (8, 128), 0)
    kt[...] = jnp.where(sub == 0, tot[0], jnp.where(sub == 1, tot[1], 0.0))

    pl.semaphore_wait(barrier, len(partners))

    kty = [rcopy(kt, kty_in.at[d], kty_send.at[d], kty_recv.at[d], at_y(d)) for d in range(1, Y)]
    for c in kty:
        c.start()
    lgc = [
        rcopy(lg.at[(h + d) % n_head], lg_in.at[d], lg_send.at[d], lg_recv.at[d], at_head(d))
        for d in range(1, n_head)
    ]
    for c in lgc:
        c.start()

    row = lax.broadcasted_iota(jnp.int32, (TOK, TOK), 0)
    col = lax.broadcasted_iota(jnp.int32, (TOK, TOK), 1)
    low = row >= col
    strict = row > col
    eye = jnp.where(row == col, 1.0, 0.0)
    lane = lax.broadcasted_iota(jnp.int32, (1, TOK), 1)

    def to_row(column):
        return jnp.sum(jnp.where(row == col, column, 0.0), axis=0, keepdims=True)

    gram, score, damp, gcol, grow, ktr, vtr = [], [], [], [], [], [], []
    for i in range(NH):
        gram.append(bdot(ks[i], ks[i], NT))
        score.append(bdot(qs[i], ks[i], NT))
        decay = ld_ref[i : i + 1, :]
        gc = jnp.sum(jnp.where(low, decay, 0.0), axis=1, keepdims=True)
        gr = to_row(gc)
        gcol.append(gc)
        grow.append(gr)
        damp.append(jnp.where(low, jnp.exp(jnp.where(low, gc - gr, 0.0)), 0.0))
        ktr.append(ks[i].T)
        vtr.append(vs[i].T)

    for c in kty:
        c.wait_recv()
    total_y = kt[...]
    for d in range(1, Y):
        total_y = total_y + kty_in[d]
    ktz[...] = total_y
    ktzc = [rcopy(ktz, ktz_in.at[d], ktz_send.at[d], ktz_recv.at[d], at_z(d)) for d in range(1, nz)]
    for c in ktzc:
        c.start()

    for c in lgc:
        c.wait_recv()
    logit = lg[h]
    for d in range(1, n_head):
        logit = logit + lg_in[d]
    beta = 1.0 / (1.0 + jnp.exp(-logit))
    brow = [beta[i : i + 1, :] for i in range(NH)]
    bcol = [jnp.sum(jnp.where(row == col, b, 0.0), axis=1, keepdims=True) for b in brow]

    for c in ktzc:
        c.wait_recv()
    total = ktz[...]
    for d in range(1, nz):
        total = total + ktz_in[d]
    limit = jnp.sqrt(total / float(n_seq * TOK) + EPSILON)

    wr_t, ur_t, rkc, rkr = [], [], [], []
    for i in range(NH):
        rc = 1.0 / jnp.maximum(jnp.sqrt(ksq[i]), limit[i : i + 1, 0:1])
        rr = to_row(rc)
        rkc.append(rc)
        rkr.append(rr)
        a = jnp.where(strict, gram[i] * damp[i] * (bcol[i] * rc) * rr, 0.0)
        inv = unit_lower_inverse(a, row, col, eye)
        wr_t.append(mm_left_exact(ktr[i], inv * (brow[i] * jnp.exp(grow[i]) * rr), NT))
        ur_t.append(mm_left_exact(vtr[i], inv * brow[i], NT))
        glast = grow[i][:, TOK - 1 : TOK]
        crow = rr * jnp.exp(glast - grow[i])
        ta[y, i] = jnp.exp(glast) * eye - mm_right_exact(wr_t[i] * crow, ks[i])
        oown[i] = mm_right_exact(ur_t[i] * crow, ks[i])

    ac = []
    for i in range(NH):
        for j, d in enumerate((1, 3)):
            hh = i if j == 0 else 1 - i
            c = rcopy(ta.at[y, hh], ta.at[y, hh], a_send.at[2 * i + j], a_recv.at[y, hh], at_y(d))
            c.start()
            ac.append(c)
    oc = []
    for d in range(1, Y):
        c = rcopy(
            oown.at[:, pl.ds(pl.multiple_of(((y + d) % Y) * SL, SL), SL), :],
            oa.at[y],
            oa_send.at[d],
            oa_recv.at[y],
            at_y(d),
        )
        c.start()
        oc.append(c)
    oa[y] = oown[:, pl.ds(pl.multiple_of(y * SL, SL), SL), :]

    left, right = (y + 3) % Y, (y + 1) % Y
    far = (y + 2) % Y

    def arrived_a(slot, hh):
        rcopy(ta.at[slot, hh], ta.at[slot, hh], a_send.at[0], a_recv.at[slot, hh], at_y(1)).wait_recv()

    arrived_a(left, 0)
    f0 = rcopy(ta.at[left, 0], ta.at[left, 0], f_send.at[0], a_recv.at[left, 0], at_y(1))
    f0.start()
    arrived_a(right, 1)
    f1 = rcopy(ta.at[right, 1], ta.at[right, 1], f_send.at[1], a_recv.at[right, 1], at_y(3))
    f1.start()

    for i in range(NH):
        rq = float(DIM) ** (-0.5) / jnp.sqrt(qsq[i] + EPSILON)
        prob = score[i] * damp[i] * rq * rkr[i]
        r_s[i] = qs[i].astype(F32) * (rq * jnp.exp(gcol[i])) - mm(prob, wr_t[i], NT)
        c_s[i] = mm(prob, ur_t[i], NT)
        gmid = grow[i][:, HALF - 1 : HALF]
        crow0 = jnp.where(lane < HALF, rkr[i] * jnp.exp(jnp.where(lane < HALF, gmid - grow[i], 0.0)), 0.0)
        t0_s[i] = jnp.exp(gmid) * eye - mm_left_exact(ktr[i], wr_t[i] * crow0, NT)
        o0_s[i] = mm_left_exact(ktr[i], ur_t[i] * crow0, NT)

    @pl.when(seg == 0)
    def _():
        for i in range(NH):
            s0t[i] = s0_ref[i].T
        seg_s[...] = s0t[:, pl.ds(pl.multiple_of(y * SL, SL), SL), :]

    arrived_a(left, 1)
    arrived_a(right, 0)
    arrived_a(far, 0)
    arrived_a(far, 1)
    for d in range(1, Y):
        slot = (y + Y - d) % Y
        rcopy(oa.at[slot], oa.at[slot], oa_send.at[0], oa_recv.at[slot], at_y(1)).wait_recv()

    for i in range(NH):
        mt, mo = ta[0, i], oa[0, i]
        et[0, i] = mt
        eo[0, i] = mo
        for k in range(1, Y):
            step = ta[k, i]
            mt, mo = mm(mt, step), mm(mo, step) + oa[k, i]
            et[k, i] = mt
            eo[k, i] = mo
    gt, go = et.at[Y - 1], eo.at[Y - 1]

    def to_b1():
        return [
            rcopy(gt, b1t, b_send.at[0], b_recv.at[0], at_z(1)),
            rcopy(go, b1o, b_send.at[1], b_recv.at[1], at_z(1)),
        ]

    def to_b2(d):
        return [
            rcopy(pt, b2t, b_send.at[2 * d], b_recv.at[2], at_z(d)),
            rcopy(po, b2o, b_send.at[2 * d + 1], b_recv.at[3], at_z(d)),
        ]

    def then(first, second, out):
        for i in range(NH):
            step = second[0][i]
            out[0][i] = mm(first[0][i], step)
            out[1][i] = mm(first[1][i], step) + second[1][i]

    @pl.when(zl % 2 == 0)
    def _():
        for c in to_b1():
            c.start()

    @pl.when(zl % 2 == 1)
    def _():
        for c in to_b1():
            c.wait_recv()
        then((b1t, b1o), (gt, go), (pt, po))

    @pl.when(zl == 1)
    def _():
        for d in (2, 1):
            for c in to_b2(d):
                c.start()

    @pl.when(zl >= 2)
    def _():
        for c in to_b2(1):
            c.wait_recv()

    @pl.when(zl == 3)
    def _():
        then((b2t, b2o), (pt, po), (p4t, p4o))

    def to_seg(d):
        return rcopy(nxt, seg_s, seg_send.at[d], seg_recv, at_z(d))

    @pl.when(seg > 0)
    def _():
        to_seg(1).wait_recv()

    @pl.when((zl == 3) & (seg < nseg - 1))
    def _():
        for i in range(NH):
            nxt[i] = mm(seg_s[i], p4t[i]) + p4o[i]
        for d in (4, 3, 2, 1):
            to_seg(d).start()

    @pl.when(zl == 3)
    def _():
        then((b2t, b2o), (b1t, b1o), (ext, exo))

    @pl.when(zl == 0)
    def _():
        sd[0] = seg_s[...]

    @pl.when(zl == 1)
    def _():
        for i in range(NH):
            sd[0, i] = mm(seg_s[i], b1t[i]) + b1o[i]

    @pl.when(zl == 2)
    def _():
        for i in range(NH):
            sd[0, i] = mm(seg_s[i], b2t[i]) + b2o[i]

    @pl.when(zl == 3)
    def _():
        for i in range(NH):
            sd[0, i] = mm(seg_s[i], ext[i]) + exo[i]

    for k in range(1, Y):
        for i in range(NH):
            sd[k, i] = mm(sd[0, i], et[k - 1, i]) + eo[k - 1, i]

    mine = pl.ds(pl.multiple_of(y * SL, SL), SL)
    sdc = [
        rcopy(sd.at[(y + d) % Y], sin.at[:, mine, :], sd_send.at[d], sd_recv.at[d], at_y(d))
        for d in range(1, Y)
    ]
    for c in sdc:
        c.start()
    sin[:, mine, :] = sd[y]
    for c in sdc:
        c.wait_recv()

    for i in range(NH):
        state_t = sin[i]
        raw = mm(r_s[i], state_t, NT) + c_s[i]
        inverse_rms = 1.0 / jnp.sqrt(jnp.mean(raw * raw, axis=1, keepdims=True) + EPSILON)
        gate = gate_ref[:, i, :].astype(F32)
        out_ref[i] = (raw * inverse_rms * (gate / (1.0 + jnp.exp(-gate)))).astype(BF16)
        st_ref[0, i] = state_t.T
        st_ref[1, i] = mm(t0_s[i], state_t, NT) + o0_s[i]

    for c in kty + lgc + ktzc + ac + oc + [f0, f1] + sdc:
        c.wait_send()

    @pl.when(zl % 2 == 0)
    def _():
        for c in to_b1():
            c.wait_send()

    @pl.when(zl == 1)
    def _():
        for d in (2, 1):
            for c in to_b2(d):
                c.wait_send()

    @pl.when((zl == 3) & (seg < nseg - 1))
    def _():
        for d in (4, 3, 2, 1):
            to_seg(d).wait_send()


def on_device(n_seq, n_head, queries, key_vectors, values, out_gate, inputs, beta_weight, log_decay, initial_state):
    nz = n_seq // Y
    vm = pl.BlockSpec(memory_space=pltpu.VMEM)
    full = pltpu.VMEM((NH, DIM, DIM), F32)
    slim = pltpu.VMEM((NH, SL, DIM), F32)
    dma = pltpu.SemaphoreType.DMA
    out, states = pl.pallas_call(
        functools.partial(kernel, n_seq, n_head),
        out_shape=(
            jax.ShapeDtypeStruct((NH, TOK, DIM), BF16),
            jax.ShapeDtypeStruct((2, NH, DIM, DIM), F32),
        ),
        in_specs=[vm] * 8,
        out_specs=(vm, vm),
        scratch_shapes=[
            pltpu.VMEM((n_head, NH, TOK), F32),
            pltpu.VMEM((n_head, NH, TOK), F32),
            pltpu.VMEM((8, 128), F32),
            pltpu.VMEM((Y, 8, 128), F32),
            pltpu.VMEM((8, 128), F32),
            pltpu.VMEM((nz, 8, 128), F32),
            pltpu.VMEM((Y, NH, DIM, DIM), F32),
            pltpu.VMEM((Y, NH, SL, DIM), F32),
            full,
            pltpu.VMEM((Y, NH, DIM, DIM), F32),
            pltpu.VMEM((Y, NH, SL, DIM), F32),
            full,
            slim,
            full,
            slim,
            full,
            slim,
            full,
            slim,
            full,
            slim,
            slim,
            slim,
            pltpu.VMEM((Y, NH, SL, DIM), F32),
            full,
            full,
            full,
            full,
            full,
            full,
            dma((n_head,)),
            dma((n_head,)),
            dma((Y,)),
            dma((Y,)),
            dma((nz,)),
            dma((nz,)),
            dma((4,)),
            dma((Y, NH)),
            dma((2,)),
            dma((Y,)),
            dma((Y,)),
            dma((6,)),
            dma((4,)),
            dma((5,)),
            dma(()),
            dma((Y,)),
            dma((Y,)),
        ],
        compiler_params=pltpu.CompilerParams(collective_id=0, has_side_effects=True),
        name="delta_layer",
    )(queries, key_vectors, values, out_gate, inputs, beta_weight, log_decay, initial_state)
    return out.transpose(1, 0, 2), states


def solution(mesh):
    in_specs = (
        P("seq", "head", None),
        P("seq", "head", None),
        P("seq", "head", None),
        P("seq", "head", None),
        P("seq", "head"),
        P(None, "head"),
        P("head", "seq"),
        P("head", None, None),
    )
    out_specs = (P("seq", "head", None), P("seq", "head", None, None))
    body = functools.partial(on_device, mesh.shape["seq"], mesh.shape["head"])
    return jax.shard_map(body, mesh=mesh, in_specs=in_specs, out_specs=out_specs, check_vma=False)
```

```python
import functools

import jax
import jax.numpy as jnp
from jax import lax
from jax.experimental import pallas as pl
from jax.experimental.pallas import tpu as pltpu
from jax.sharding import PartitionSpec as P

MESH = pl.DeviceIdType.MESH
F32 = jnp.float32
BF16 = jnp.bfloat16
EPSILON = 1e-06
Y = 4
Z4 = 4
TOK = 128
HALF = 64
DIM = 128
SL = DIM // Y
NH = 2

NN = (((1,), (0,)), ((), ()))
NT = (((1,), (1,)), ((), ()))


def bdot(a, b, dims):
    return lax.dot_general(a, b, dims, preferred_element_type=F32)


def split(x):
    high = x.astype(BF16)
    return high, (x - high.astype(F32)).astype(BF16)


def mm(a, b, dims=NN):
    ah, al = split(a)
    bh, bl = split(b)
    return bdot(ah, bh, dims) + (bdot(al, bh, dims) + bdot(ah, bl, dims))


def mm_right_exact(a, b, dims=NN):
    ah, al = split(a)
    return bdot(ah, b, dims) + bdot(al, b, dims)


def mm_left_exact(a, b, dims=NN):
    bh, bl = split(b)
    return bdot(a, bh, dims) + bdot(a, bl, dims)


def unit_lower_inverse(strict_part, row, col, eye):
    def same(size):
        return (row // size) == (col // size)

    base = jnp.where(same(8), strict_part, 0.0)
    square = mm(base, base)
    cube = mm(base, square)
    fourth = mm(square, square)
    part = eye - base + square - cube
    inverse = part + mm(part, fourth)
    size = 8
    while size < TOK:
        below = jnp.where(same(2 * size) & jnp.logical_not(same(size)), strict_part, 0.0)
        inverse = inverse - mm(inverse, mm(below, inverse))
        size *= 2
    return inverse


def kernel(
    n_seq,
    n_head,
    q_ref,
    k_ref,
    v_ref,
    x_ref,
    w_ref,
    ld_ref,
    s0_ref,
    start_s,
    r_s,
    c_s,
    t0_s,
    o0_s,
    lg,
    lg_in,
    kt,
    kty_in,
    ktz,
    ktz_in,
    ta,
    oa,
    oown,
    et,
    eo,
    b1t,
    b1o,
    b2t,
    b2o,
    pt,
    po,
    p4t,
    p4o,
    ext,
    exo,
    seg_s,
    nxt,
    sd,
    sin,
    s0t,
    lg_send,
    lg_recv,
    kty_send,
    kty_recv,
    ktz_send,
    ktz_recv,
    a_send,
    a_recv,
    f_send,
    oa_send,
    oa_recv,
    b_send,
    b_recv,
    seg_send,
    seg_recv,
    sd_send,
    sd_recv,
):
    nz = n_seq // Y
    nseg = nz // Z4
    s = lax.axis_index("seq")
    h = lax.axis_index("head")
    z = s // Y
    y = s % Y
    zl = z % Z4
    seg = z // Z4

    def at_y(d):
        return {"seq": z * Y + (y + d) % Y, "head": h}

    def at_z(d):
        return {"seq": ((z + d) % nz) * Y + y, "head": h}

    def at_head(d):
        return {"seq": s, "head": (h + d) % n_head}

    def rcopy(src, dst, ssem, rsem, dev):
        return pltpu.make_async_remote_copy(
            src_ref=src, dst_ref=dst, send_sem=ssem, recv_sem=rsem, device_id=dev, device_id_type=MESH
        )

    barrier = pltpu.get_barrier_semaphore()
    partners = (
        [at_head(d) for d in range(1, n_head)]
        + [at_y(d) for d in range(1, Y)]
        + [at_z(d) for d in range(1, nz)]
    )
    for dev in partners:
        pl.semaphore_signal(barrier, inc=1, device_id=dev, device_id_type=MESH)

    logits = bdot(w_ref[...], x_ref[...], NT)
    for p in range(n_head):
        lg[p] = logits[NH * p : NH * p + NH]
    ks = [k_ref[:, i, :] for i in range(NH)]
    qs = [q_ref[:, i, :] for i in range(NH)]
    vs = [v_ref[:, i, :] for i in range(NH)]
    ksq = [jnp.sum(jnp.square(k.astype(F32)), axis=1, keepdims=True) for k in ks]
    qsq = [jnp.sum(jnp.square(q.astype(F32)), axis=1, keepdims=True) for q in qs]
    tot = [jnp.sum(a, axis=0, keepdims=True) for a in ksq]
    sub = lax.broadcasted_iota(jnp.int32, (8, 128), 0)
    kt[...] = jnp.where(sub == 0, tot[0], jnp.where(sub == 1, tot[1], 0.0))

    pl.semaphore_wait(barrier, len(partners))

    kty = [rcopy(kt, kty_in.at[d], kty_send.at[d], kty_recv.at[d], at_y(d)) for d in range(1, Y)]
    for c in kty:
        c.start()
    lgc = [
        rcopy(lg.at[(h + d) % n_head], lg_in.at[d], lg_send.at[d], lg_recv.at[d], at_head(d))
        for d in range(1, n_head)
    ]
    for c in lgc:
        c.start()

    row = lax.broadcasted_iota(jnp.int32, (TOK, TOK), 0)
    col = lax.broadcasted_iota(jnp.int32, (TOK, TOK), 1)
    low = row >= col
    strict = row > col
    eye = jnp.where(row == col, 1.0, 0.0)
    lane = lax.broadcasted_iota(jnp.int32, (1, TOK), 1)

    def to_row(column):
        return jnp.sum(jnp.where(row == col, column, 0.0), axis=0, keepdims=True)

    gram, score, damp, gcol, grow, ktr, vtr = [], [], [], [], [], [], []
    for i in range(NH):
        gram.append(bdot(ks[i], ks[i], NT))
        score.append(bdot(qs[i], ks[i], NT))
        decay = ld_ref[i : i + 1, :]
        gc = jnp.sum(jnp.where(low, decay, 0.0), axis=1, keepdims=True)
        gr = to_row(gc)
        gcol.append(gc)
        grow.append(gr)
        damp.append(jnp.where(low, jnp.exp(jnp.where(low, gc - gr, 0.0)), 0.0))
        ktr.append(ks[i].T)
        vtr.append(vs[i].T)

    for c in kty:
        c.wait_recv()
    total_y = kt[...]
    for d in range(1, Y):
        total_y = total_y + kty_in[d]
    ktz[...] = total_y
    ktzc = [rcopy(ktz, ktz_in.at[d], ktz_send.at[d], ktz_recv.at[d], at_z(d)) for d in range(1, nz)]
    for c in ktzc:
        c.start()

    for c in lgc:
        c.wait_recv()
    logit = lg[h]
    for d in range(1, n_head):
        logit = logit + lg_in[d]
    beta = 1.0 / (1.0 + jnp.exp(-logit))
    brow = [beta[i : i + 1, :] for i in range(NH)]
    bcol = [jnp.sum(jnp.where(row == col, b, 0.0), axis=1, keepdims=True) for b in brow]

    for c in ktzc:
        c.wait_recv()
    total = ktz[...]
    for d in range(1, nz):
        total = total + ktz_in[d]
    limit = jnp.sqrt(total / float(n_seq * TOK) + EPSILON)

    wr_t, ur_t, rkc, rkr = [], [], [], []
    for i in range(NH):
        rc = 1.0 / jnp.maximum(jnp.sqrt(ksq[i]), limit[i : i + 1, 0:1])
        rr = to_row(rc)
        rkc.append(rc)
        rkr.append(rr)
        a = jnp.where(strict, gram[i] * damp[i] * (bcol[i] * rc) * rr, 0.0)
        inv = unit_lower_inverse(a, row, col, eye)
        wr_t.append(mm_left_exact(ktr[i], inv * (brow[i] * jnp.exp(grow[i]) * rr), NT))
        ur_t.append(mm_left_exact(vtr[i], inv * brow[i], NT))
        glast = grow[i][:, TOK - 1 : TOK]
        crow = rr * jnp.exp(glast - grow[i])
        ta[y, i] = jnp.exp(glast) * eye - mm_right_exact(wr_t[i] * crow, ks[i])
        oown[i] = mm_right_exact(ur_t[i] * crow, ks[i])

    ac = []
    for i in range(NH):
        for j, d in enumerate((1, 3)):
            hh = i if j == 0 else 1 - i
            c = rcopy(ta.at[y, hh], ta.at[y, hh], a_send.at[2 * i + j], a_recv.at[y, hh], at_y(d))
            c.start()
            ac.append(c)
    oc = []
    for d in range(1, Y):
        c = rcopy(
            oown.at[:, pl.ds(pl.multiple_of(((y + d) % Y) * SL, SL), SL), :],
            oa.at[y],
            oa_send.at[d],
            oa_recv.at[y],
            at_y(d),
        )
        c.start()
        oc.append(c)
    oa[y] = oown[:, pl.ds(pl.multiple_of(y * SL, SL), SL), :]

    left, right = (y + 3) % Y, (y + 1) % Y
    far = (y + 2) % Y

    def arrived_a(slot, hh):
        rcopy(ta.at[slot, hh], ta.at[slot, hh], a_send.at[0], a_recv.at[slot, hh], at_y(1)).wait_recv()

    arrived_a(left, 0)
    f0 = rcopy(ta.at[left, 0], ta.at[left, 0], f_send.at[0], a_recv.at[left, 0], at_y(1))
    f0.start()
    arrived_a(right, 1)
    f1 = rcopy(ta.at[right, 1], ta.at[right, 1], f_send.at[1], a_recv.at[right, 1], at_y(3))
    f1.start()

    for i in range(NH):
        rq = float(DIM) ** (-0.5) / jnp.sqrt(qsq[i] + EPSILON)
        prob = score[i] * damp[i] * rq * rkr[i]
        r_s[i] = qs[i].astype(F32) * (rq * jnp.exp(gcol[i])) - mm(prob, wr_t[i], NT)
        c_s[i] = mm(prob, ur_t[i], NT)
        gmid = grow[i][:, HALF - 1 : HALF]
        crow0 = jnp.where(lane < HALF, rkr[i] * jnp.exp(jnp.where(lane < HALF, gmid - grow[i], 0.0)), 0.0)
        t0_s[i] = jnp.exp(gmid) * eye - mm_left_exact(ktr[i], wr_t[i] * crow0, NT)
        o0_s[i] = mm_left_exact(ktr[i], ur_t[i] * crow0, NT)

    @pl.when(z == 0)
    def _():
        for i in range(NH):
            s0t[i] = s0_ref[i].T
        seg_s[...] = s0t[:, pl.ds(pl.multiple_of(y * SL, SL), SL), :]

    arrived_a(left, 1)
    arrived_a(right, 0)
    arrived_a(far, 0)
    arrived_a(far, 1)
    for d in range(1, Y):
        slot = (y + Y - d) % Y
        rcopy(oa.at[slot], oa.at[slot], oa_send.at[0], oa_recv.at[slot], at_y(1)).wait_recv()

    for i in range(NH):
        mt, mo = ta[0, i], oa[0, i]
        et[0, i] = mt
        eo[0, i] = mo
        for k in range(1, Y):
            step = ta[k, i]
            mt, mo = mm(mt, step), mm(mo, step) + oa[k, i]
            et[k, i] = mt
            eo[k, i] = mo
    gt, go = et.at[Y - 1], eo.at[Y - 1]
    first = seg == 0

    def to_b1(i):
        return [
            rcopy(gt.at[i], b1t.at[i], b_send.at[2 * i], b_recv.at[2 * i], at_z(1)),
            rcopy(go.at[i], b1o.at[i], b_send.at[2 * i + 1], b_recv.at[2 * i + 1], at_z(1)),
        ]

    def to_b2(d, i):
        k = 4 * d + 2 * i
        return [
            rcopy(pt.at[i], b2t.at[i], b_send.at[k], b_recv.at[4 + 2 * i], at_z(d)),
            rcopy(po.at[i], b2o.at[i], b_send.at[k + 1], b_recv.at[5 + 2 * i], at_z(d)),
        ]

    def then(first_map, second_map, out, i):
        step = second_map[0][i]
        out[0][i] = mm(first_map[0][i], step)
        out[1][i] = mm(first_map[1][i], step) + second_map[1][i]

    def apply(state, by, out, i):
        out[i] = mm(state[i], by[0][i]) + by[1][i]

    sends_b1 = (zl == 2) | ((zl == 0) & (seg > 0))
    takes_b1 = (zl == 3) | ((zl == 1) & (seg > 0))
    sends_b2 = (zl == 1) & (seg > 0)
    takes_b2 = (zl >= 2) & (seg > 0)

    def to_next(d):
        return rcopy(nxt, seg_s, seg_send.at[d], seg_recv, at_z(d))

    @pl.when(z == 0)
    def _():
        for i in range(NH):
            apply(seg_s, (gt, go), nxt, i)
        to_next(1).start()

    @pl.when(sends_b1)
    def _():
        for i in range(NH):
            for c in to_b1(i):
                c.start()

    @pl.when(takes_b1)
    def _():
        for i in range(NH):
            for c in to_b1(i):
                c.wait_recv()
            then((b1t, b1o), (gt, go), (pt, po), i)

            @pl.when(sends_b2)
            def _(i=i):
                for c in to_b2(2, i):
                    c.start()

    @pl.when(sends_b2)
    def _():
        for i in range(NH):
            for c in to_b2(1, i):
                c.start()

    @pl.when(takes_b2)
    def _():
        for i in range(NH):
            for c in to_b2(1, i):
                c.wait_recv()

    @pl.when((zl == 3) & (seg > 0))
    def _():
        for i in range(NH):
            then((b2t, b2o), (pt, po), (p4t, p4o), i)
        for i in range(NH):
            then((b2t, b2o), (b1t, b1o), (ext, exo), i)

    @pl.when(z > 0)
    def _():
        to_next(1).wait_recv()

    @pl.when(z == 1)
    def _():
        for i in range(NH):
            apply(seg_s, (gt, go), nxt, i)
        for d in (2, 1):
            to_next(d).start()

    if nseg > 1:

        @pl.when(z == 3)
        def _():
            for i in range(NH):
                apply(seg_s, (pt, po), nxt, i)

        @pl.when((zl == 3) & (seg > 0) & (seg < nseg - 1))
        def _():
            for i in range(NH):
                apply(seg_s, (p4t, p4o), nxt, i)

        @pl.when((zl == 3) & (seg < nseg - 1))
        def _():
            for d in (4, 3, 2, 1):
                to_next(d).start()

    start = sd.at[0]

    @pl.when((zl == 0) | (first & (zl < 3)))
    def _():
        sd[0] = seg_s[...]

    @pl.when(sends_b2 | (z == 3))
    def _():
        for i in range(NH):
            apply(seg_s, (b1t, b1o), start, i)

    @pl.when((zl == 2) & (seg > 0))
    def _():
        for i in range(NH):
            apply(seg_s, (b2t, b2o), start, i)

    @pl.when((zl == 3) & (seg > 0))
    def _():
        for i in range(NH):
            apply(seg_s, (ext, exo), start, i)

    for k in range(1, Y):
        for i in range(NH):
            sd[k, i] = mm(sd[0, i], et[k - 1, i]) + eo[k - 1, i]

    mine = pl.ds(pl.multiple_of(y * SL, SL), SL)
    sdc = [
        rcopy(sd.at[(y + d) % Y], sin.at[:, mine, :], sd_send.at[d], sd_recv.at[d], at_y(d))
        for d in range(1, Y)
    ]
    for c in sdc:
        c.start()
    sin[:, mine, :] = sd[y]
    for c in sdc:
        c.wait_recv()
    start_s[...] = sin[...]

    for c in kty + lgc + ktzc + ac + oc + [f0, f1] + sdc:
        c.wait_send()

    @pl.when(sends_b1)
    def _():
        for i in range(NH):
            for c in to_b1(i):
                c.wait_send()

    @pl.when(sends_b2)
    def _():
        for d in (2, 1):
            for i in range(NH):
                for c in to_b2(d, i):
                    c.wait_send()

    @pl.when(z == 0)
    def _():
        to_next(1).wait_send()

    @pl.when(z == 1)
    def _():
        for d in (2, 1):
            to_next(d).wait_send()

    if nseg > 1:

        @pl.when((zl == 3) & (seg < nseg - 1))
        def _():
            for d in (4, 3, 2, 1):
                to_next(d).wait_send()


def finish(gate_ref, sin, r_s, c_s, t0_s, o0_s, out_ref, st_ref):
    gated = []
    for i in range(NH):
        state_t = sin[i]
        raw = mm(r_s[i], state_t, NT) + c_s[i]
        inverse_rms = 1.0 / jnp.sqrt(jnp.mean(raw * raw, axis=1, keepdims=True) + EPSILON)
        gate = gate_ref[:, i, :].astype(F32)
        gated.append(raw * inverse_rms * (gate / (1.0 + jnp.exp(-gate))))
        st_ref[0, i] = state_t.T
        st_ref[1, i] = mm(t0_s[i], state_t, NT) + o0_s[i]
    for i in range(NH):
        out_ref[:, i, :] = gated[i].astype(BF16)


def on_device(n_seq, n_head, queries, key_vectors, values, out_gate, inputs, beta_weight, log_decay, initial_state):
    nz = n_seq // Y
    vm = pl.BlockSpec(memory_space=pltpu.VMEM)
    full = pltpu.VMEM((NH, DIM, DIM), F32)
    slim = pltpu.VMEM((NH, SL, DIM), F32)
    dma = pltpu.SemaphoreType.DMA
    parts = pl.pallas_call(
        functools.partial(kernel, n_seq, n_head),
        out_shape=[full] * 5,
        in_specs=[vm] * 7,
        out_specs=[vm] * 5,
        scratch_shapes=[
            pltpu.VMEM((n_head, NH, TOK), F32),
            pltpu.VMEM((n_head, NH, TOK), F32),
            pltpu.VMEM((8, 128), F32),
            pltpu.VMEM((Y, 8, 128), F32),
            pltpu.VMEM((8, 128), F32),
            pltpu.VMEM((nz, 8, 128), F32),
            pltpu.VMEM((Y, NH, DIM, DIM), F32),
            pltpu.VMEM((Y, NH, SL, DIM), F32),
            full,
            pltpu.VMEM((Y, NH, DIM, DIM), F32),
            pltpu.VMEM((Y, NH, SL, DIM), F32),
            full,
            slim,
            full,
            slim,
            full,
            slim,
            full,
            slim,
            full,
            slim,
            slim,
            slim,
            pltpu.VMEM((Y, NH, SL, DIM), F32),
            full,
            full,
            dma((n_head,)),
            dma((n_head,)),
            dma((Y,)),
            dma((Y,)),
            dma((nz,)),
            dma((nz,)),
            dma((4,)),
            dma((Y, NH)),
            dma((2,)),
            dma((Y,)),
            dma((Y,)),
            dma((12,)),
            dma((8,)),
            dma((5,)),
            dma(()),
            dma((Y,)),
            dma((Y,)),
        ],
        compiler_params=pltpu.CompilerParams(collective_id=0, has_side_effects=True),
        name="delta_layer",
    )(queries, key_vectors, values, inputs, beta_weight, log_decay, initial_state)
    return pl.pallas_call(
        finish,
        out_shape=(
            jax.ShapeDtypeStruct((TOK, NH, DIM), BF16),
            jax.ShapeDtypeStruct((2, NH, DIM, DIM), F32),
        ),
        in_specs=[vm] * 6,
        out_specs=(vm, vm),
        name="delta_output",
    )(out_gate, *[pltpu.with_memory_space_constraint(a, pltpu.VMEM) for a in parts])


def solution(mesh):
    in_specs = (
        P("seq", "head", None),
        P("seq", "head", None),
        P("seq", "head", None),
        P("seq", "head", None),
        P("seq", "head"),
        P(None, "head"),
        P("head", "seq"),
        P("head", None, None),
    )
    out_specs = (P("seq", "head", None), P("seq", "head", None, None))
    body = functools.partial(on_device, mesh.shape["seq"], mesh.shape["head"])
    return jax.shard_map(body, mesh=mesh, in_specs=in_specs, out_specs=out_specs, check_vma=False)
```
